256 devices in a mesh: dp: 4 (over y), ctx: 64 (over x, z, core).
Axes of the slice: x: 4, y: 4, z: 8, core: 2. Of those that a mesh axis runs over, the one named last changes fastest.
Arguments:
- hidden: bfloat16 [4, 32768, 8192], P('dp', 'ctx'), may hold values from -8 to 8
- norm_gain: float32 [8192], replicated, may hold values from 0.3 to 5.2
- cotangent: bfloat16 [4, 32768, 512], P('dp', 'ctx'), may hold values from -30 to 30
- loss_weight: float32 [4], P('dp'), may hold values from 0.08 to 5
Outputs:
- clipped_grad: float32 [8192, 512], P('ctx', 'dp')
The draws below stay inside these ranges and needn't reach their ends.
All inputs are finite; a program needn't handle non-finite values.
Results may differ from the reference program's by a relative error of at most 0.0022.
Values may be sent and summed in bfloat16 or wider, within the bound.
No kernel may reach another device: no remote copies, remote signals or barrier semaphores. Data moves between devices by JAX's collectives and lax.ppermute only.
A program may use at most 64 MiB of HBM per device.

```python
import math
from functools import partial
import jax
import jax.numpy as jnp
from jax import lax

D = 8192
OUT = 512
LENGTH = 32768
EXAMPLES = 4


def draw_hidden(key, part):
    base_key = jax.random.fold_in(key, 41)
    mean_key = jax.random.fold_in(key, 42)
    shared = jax.random.truncated_normal(mean_key, -4.0, 4.0, (EXAMPLES, 1, D), jnp.float32)
    base = jax.random.truncated_normal(base_key, -6.0, 6.0, (EXAMPLES, LENGTH, D), jnp.float32)
    return (base + 0.5 * shared).astype(jnp.bfloat16)


def draw_norm_gain(key, part):
    first_key = jax.random.fold_in(key, 11)
    ramp = jnp.sqrt(1.0 + 2.0 * jnp.arange(D, dtype=jnp.float32) / D)
    rough = jnp.exp(jax.random.uniform(first_key, (D,), jnp.float32, math.log(0.3), math.log(3.0)))
    return (ramp * rough).astype(jnp.float32)


def draw_cotangent(key, part):
    scale_key = jax.random.fold_in(key, 21)
    base_key = jax.random.fold_in(key, 22)
    common_key = jax.random.fold_in(key, 23)
    column_scale = jnp.exp(jax.random.uniform(scale_key, (OUT,), jnp.float32, math.log(0.3), math.log(3.0)))
    shared = jax.random.truncated_normal(common_key, -6.0, 6.0, (EXAMPLES, 1, OUT), jnp.float32)
    base = jax.random.truncated_normal(base_key, -6.0, 6.0, (EXAMPLES, LENGTH, OUT), jnp.float32)
    base = base + 2.0 / math.sqrt(LENGTH) * shared
    return (base * column_scale).astype(jnp.bfloat16)


def draw_loss_weight(key, part):
    order_key = jax.random.fold_in(key, 31)
    small_key = jax.random.fold_in(key, 32)
    large_key = jax.random.fold_in(key, 33)
    order = jax.random.permutation(order_key, EXAMPLES)
    small = jnp.exp(jax.random.uniform(small_key, (EXAMPLES,), jnp.float32, math.log(0.08), math.log(0.2)))
    large = jnp.exp(jax.random.uniform(large_key, (EXAMPLES,), jnp.float32, math.log(1.5), math.log(5.0)))
    return jnp.where(order % 2 == 0, small, large).astype(jnp.float32)


def setup_inputs(seed: int = 0) -> dict:
    arg_keys = jax.random.split(jax.random.key(seed), 5)
    hidden = draw_hidden(jax.random.fold_in(arg_keys[4], 71), 0)
    norm_gain = draw_norm_gain(jax.random.fold_in(arg_keys[4], 71), 0)
    cotangent = draw_cotangent(jax.random.fold_in(arg_keys[4], 71), 0)
    loss_weight = draw_loss_weight(jax.random.fold_in(arg_keys[4], 71), 0)
    return dict(hidden=hidden, norm_gain=norm_gain, cotangent=cotangent, loss_weight=loss_weight)


def per_example(gain_vector, bundle):
    values, upstream, weight = bundle
    widened = values.astype(jnp.float32)
    scale = lax.rsqrt(lax.optimization_barrier(jnp.mean(widened * widened, axis=1, keepdims=True)) + 1e-05)
    normed = (widened * scale * gain_vector).astype(jnp.bfloat16)
    product = lax.dot_general(normed, upstream, (((0,), (0,)), ((), ())), preferred_element_type=jnp.float32)
    return product * (weight / math.sqrt(LENGTH))

def reference(hidden, norm_gain, cotangent, loss_weight):
    grads = lax.map(partial(per_example, norm_gain), (hidden, cotangent, loss_weight))
    squares = lax.optimization_barrier(jnp.sum(grads * grads, axis=(1, 2)))
    clip_bound = math.sqrt(D * OUT)
    factor = jnp.minimum(1.0, clip_bound * lax.rsqrt(squares + 1e-06))
    return lax.optimization_barrier(jnp.sum(factor[:, None, None] * grads, axis=0))
```

```python
import functools
import math

import jax
import jax.numpy as jnp
from jax import lax
from jax.experimental import pallas as pl
from jax.experimental.pallas import tpu as pltpu
from jax.sharding import Mesh
from jax.sharding import PartitionSpec as P


X, Z, CORE, DP = 4, 8, 2, 4
LANE = 128
WIRE = jnp.bfloat16
WIRE_TOP = 15.0
TAIL = 16
VMEM = pltpu.VMEM
F32 = jnp.float32


def call(kernel, out_shape, in_specs, out_specs, scalars=0, grid=(), scratch=(), flops=0, moved=0, mib=12):
    return pl.pallas_call(
        kernel,
        out_shape=out_shape,
        compiler_params=pltpu.CompilerParams(vmem_limit_bytes=mib << 20),
        grid_spec=pltpu.PrefetchScalarGridSpec(
            num_scalar_prefetch=scalars,
            grid=grid,
            in_specs=in_specs,
            out_specs=out_specs,
            scratch_shapes=list(scratch),
        ),
        cost_estimate=pl.CostEstimate(flops=flops, bytes_accessed=moved, transcendentals=0),
    )


def whole():
    return pl.BlockSpec(memory_space=VMEM)


def prep_kernel(core_ref, hidden_ref, cot_ref, send_ref, scale_ref, top_ref):
    step = pl.program_id(0)
    rows, features = hidden_ref.shape
    other = 1 - core_ref[0]
    tiles = features // LANE
    total = jnp.zeros((rows, LANE), F32)
    for i in range(tiles):
        v = hidden_ref[:, i * LANE : (i + 1) * LANE].astype(F32)
        total = total + v * v
    mean = jnp.sum(total, axis=1, keepdims=True) * (1.0 / features)
    scale = lax.rsqrt(mean + 1e-05)
    at = pl.multiple_of(step * rows, rows)
    scale_ref[pl.ds(at, rows), :] = jnp.broadcast_to(scale, (rows, LANE))
    for i in range(tiles // 2):
        src = pl.multiple_of((2 * i + other) * LANE, LANE)
        send_ref[:, i * LANE : (i + 1) * LANE] = hidden_ref[:, pl.ds(src, LANE)]
    largest = jnp.max(jnp.abs(cot_ref[...].astype(F32)), axis=0, keepdims=True)
    lanes = largest[:, :LANE]
    for i in range(1, largest.shape[1] // LANE):
        lanes = jnp.maximum(lanes, largest[:, i * LANE : (i + 1) * LANE])

    @pl.when(step == 0)
    def _():
        top_ref[...] = jnp.zeros_like(top_ref)

    top_ref[...] = jnp.maximum(top_ref[...], jnp.broadcast_to(lanes, top_ref.shape))
    last = scale_ref.shape[0] - 8
    scale_ref[last:, :] = top_ref[...]


def prep(hidden, cot, core):
    tokens, features = hidden.shape
    steps = 8
    rows = tokens // steps
    return call(
        prep_kernel,
        (
            jax.ShapeDtypeStruct((tokens, features // 2), hidden.dtype),
            jax.ShapeDtypeStruct((tokens + 8, LANE), F32),
        ),
        [
            pl.BlockSpec((rows, features), lambda i, s: (i, 0)),
            pl.BlockSpec((rows, cot.shape[1]), lambda i, s: (i, 0)),
        ],
        (
            pl.BlockSpec((rows, features // 2), lambda i, s: (i, 0)),
            pl.BlockSpec((tokens + 8, LANE), lambda i, s: (0, 0)),
        ),
        scalars=1,
        grid=(steps,),
        scratch=[VMEM((8, LANE), F32)],
        flops=2 * tokens * features,
        moved=3 * tokens * features,
        mib=56,
    )(core, hidden, cot)


def product_kernel(keep, at_ref, *refs):
    own = refs[:2]
    par_ref, so_ref, sp_ref, gain_ref, cto_ref, ctp_ref, a_ref, b_ref, normed = refs[2:]
    step = pl.program_id(0)
    tokens = par_ref.shape[0]
    half = cto_ref.shape[0] // 2
    first = at_ref[0] * (2 * Z) + at_ref[1] + 4 * step
    so = so_ref[:tokens, :]
    sp = sp_ref[:tokens, :]
    for i in range(2):
        g = gain_ref[pl.ds(first + 2 * i, 1), :]
        lanes = slice(i * LANE, (i + 1) * LANE)
        normed[:tokens, lanes] = (own[i][...].astype(F32) * so * g).astype(jnp.bfloat16)
        normed[tokens:, lanes] = (par_ref[:, lanes].astype(F32) * sp * g).astype(jnp.bfloat16)
    features = gain_ref.shape[0] * gain_ref.shape[1]
    top = jnp.maximum(jnp.max(so_ref[tokens:, :]), jnp.max(sp_ref[tokens:, :]))
    steepest = jnp.max(jnp.abs(gain_ref[...]))
    bound = jnp.maximum(2.0 * tokens * math.sqrt(features) * top * steepest, 1e-30)
    power = jnp.ceil(jnp.log(jnp.full((1, LANE), bound, F32)) * (1.0 / math.log(2.0))) - WIRE_TOP
    down = jnp.exp(power * -math.log(2.0))
    out = jnp.dot(cto_ref[...], normed[:tokens, :], preferred_element_type=F32)
    out = out + jnp.dot(ctp_ref[...], normed[tokens:, :], preferred_element_type=F32)
    for i in range(2):
        at = pl.multiple_of((2 * step + i) * half, half)
        tile = out[:, i * LANE : (i + 1) * LANE]
        if not keep:
            tile = tile * down
        a_ref[pl.ds(at, half), :] = tile[:half].astype(a_ref.dtype)
        b_ref[pl.ds(at, half), :] = tile[half:].astype(b_ref.dtype)
    tail = jnp.broadcast_to(power, (TAIL, LANE))
    a_ref[Z * half :, :] = tail.astype(a_ref.dtype)
    b_ref[Z * half :, :] = tail.astype(b_ref.dtype)


def product(hidden, par, so, sp, gain, cto, ctp, at, keep):
    tokens = par.shape[0]
    outs = cto.shape[0]
    half = outs // 2
    dtype = F32 if keep else WIRE
    shape = jax.ShapeDtypeStruct((Z * half + TAIL, LANE), dtype)
    fixed = lambda a: pl.BlockSpec(a.shape, lambda i, s: (0, 0))
    tile = lambda k: pl.BlockSpec((tokens, LANE), lambda i, s: (0, s[0] * (2 * Z) + s[1] + 4 * i + 2 * k))
    out = pl.BlockSpec(shape.shape, lambda i, s: (0, 0))
    return call(
        functools.partial(product_kernel, keep),
        (shape, shape),
        [
            tile(0),
            tile(1),
            pl.BlockSpec((tokens, 2 * LANE), lambda i, s: (0, s[0] * (Z // 2) + i)),
            fixed(so),
            fixed(sp),
            fixed(gain),
            fixed(cto),
            fixed(ctp),
        ],
        (out, out),
        scalars=1,
        grid=(Z // 2,),
        scratch=[VMEM((2 * tokens, 2 * LANE), jnp.bfloat16)],
        flops=2 * outs * 2 * tokens * Z * LANE,
        moved=4 * tokens * Z * LANE + 4 * outs * Z * LANE,
        mib=52,
    )(at, hidden, hidden, par, so, sp, gain, cto, ctp)


def up(power):
    return jnp.exp(power.astype(F32) * math.log(2.0))


def gather_kernel(own_ref, r1_ref, r2_ref, r3_ref, out_ref):
    rows = own_ref.shape[0] - TAIL
    half = rows // Z
    power = own_ref[rows : rows + 1, :]
    scales = []
    for r in (r1_ref, r2_ref, r3_ref):
        p = r[rows:, :].astype(F32)[:1, :]
        scales.append(up(p))
        power = jnp.maximum(power, p)
    power = power + 2.0
    down = jnp.exp(power * -math.log(2.0))
    tail = jnp.broadcast_to(power, (TAIL, LANE)).astype(out_ref.dtype)
    for j in range(Z):
        at = slice(j * half, (j + 1) * half)
        total = own_ref[at, :]
        for r, s in zip((r1_ref, r2_ref, r3_ref), scales):
            total = total + r[at, :].astype(F32) * s
        out_ref[j, :half, :] = (total * down).astype(out_ref.dtype)
        out_ref[j, half:, :] = tail


def gather(own, r1, r2, r3):
    half = (own.shape[0] - TAIL) // Z
    return call(
        gather_kernel,
        jax.ShapeDtypeStruct((Z, half + TAIL, LANE), WIRE),
        [whole()] * 4,
        whole(),
        flops=8 * own.size,
        moved=12 * own.size,
    )(own, r1, r2, r3)


def finish_kernel(at_ref, weight_ref, a_ref, b_ref, *refs):
    outs, squares_ref, tile = refs[:DP], refs[DP], refs[DP + 1]
    half = a_ref.shape[1] - TAIL
    weight = weight_ref[0]
    squares = jnp.zeros((1, LANE), F32)
    for n, r in enumerate((a_ref, b_ref)):
        scales = [up(r[j, half:, :].astype(F32)[:1, :]) * weight for j in range(Z)]
        total = r[0, :half, :].astype(F32) * scales[0]
        for j in range(1, Z):
            total = total + r[j, :half, :].astype(F32) * scales[j]
        tile[n * half : (n + 1) * half, :] = total
        squares = squares + jnp.sum(total * total, axis=0, keepdims=True)
    rows = 2 * half // DP
    for k in range(DP):
        owner = jnp.bitwise_and(at_ref[0] + k, DP - 1)
        outs[k][...] = tile[pl.ds(pl.multiple_of(owner * rows, rows), rows), :]
    squares_ref[...] = jnp.broadcast_to(squares[None], squares_ref.shape)


def finish(a, b, dp, weight):
    half = a.shape[1] - TAIL
    rows = 2 * half // DP
    block = jax.ShapeDtypeStruct((rows, LANE), F32)
    return call(
        finish_kernel,
        (block,) * DP + (jax.ShapeDtypeStruct((Z * CORE, 1, LANE), F32),),
        [pl.BlockSpec(memory_space=pltpu.SMEM), whole(), whole()],
        (whole(),) * (DP + 1),
        scalars=1,
        scratch=[VMEM((2 * half, LANE), F32)],
        flops=4 * a.size,
        moved=4 * a.size,
    )(dp, weight, a, b)


def pass_kernel(in_ref, out_ref):
    out_ref[...] = jnp.broadcast_to(jnp.sum(in_ref[...], axis=0, keepdims=True), out_ref.shape)


def combine_kernel(clip_bound, at_ref, squares_ref, *refs):
    blocks, out_ref = refs[:DP], refs[DP]
    total = None
    for k in range(DP):
        example = jnp.bitwise_and(at_ref[0] + DP - k, DP - 1)
        squares = jnp.sum(squares_ref[pl.ds(example * X, X)])
        factor = jnp.minimum(1.0, clip_bound * lax.rsqrt(jnp.full((1, LANE), squares, F32) + 1e-06))
        term = blocks[k][...] * factor
        total = term if total is None else total + term
    out_ref[...] = total.T


def turn(n, k):
    return [(i, (i + k) % n) for i in range(n)]


def per_device(hidden, norm_gain, cotangent, loss_weight):
    hidden, cot = hidden[0], cotangent[0]
    tokens, features = hidden.shape
    outs = cot.shape[1]
    doc_length = tokens * X * Z * CORE
    x, core, dp = (lax.axis_index(n).astype(jnp.int32) for n in ("x", "core", "dp"))
    swap = functools.partial(lax.ppermute, axis_name="core", perm=turn(CORE, 1))
    send, so = prep(hidden, cot, core[None])
    par = swap(send)
    cto = cot.T
    ctp = swap(cto)
    sp = swap(so)
    gain = norm_gain.reshape(features // LANE, LANE)
    weight = loss_weight * (1.0 / math.sqrt(doc_length))

    def block(k):
        at = jnp.stack([jnp.bitwise_and(x + k, X - 1), core])
        return product(hidden, par, so, sp, gain, cto, ctp, at, k == 0)

    blocks = {k: block(k) for k in (1, 3, 2, 0)}
    summed = []
    for chunk in range(2):
        arrived = [lax.ppermute(blocks[k][chunk], "x", turn(X, k)) for k in (1, 3, 2)]
        ready = gather(blocks[0][chunk], *arrived)
        summed.append(lax.all_to_all(ready, "z", split_axis=0, concat_axis=0, tiled=True))
    *tiles, squares = finish(*summed, dp[None], weight)
    arrived = [tiles[0]] + [lax.ppermute(tiles[k], "dp", turn(DP, k)) for k in range(1, DP)]
    squares = lax.all_to_all(squares, ("z", "core"), split_axis=0, concat_axis=0, tiled=True)
    squares = call(pass_kernel, jax.ShapeDtypeStruct((DP * X, 1, LANE), F32), [whole()], whole())(squares)
    squares = lax.all_to_all(squares, ("dp", "x"), split_axis=0, concat_axis=0, tiled=True)
    clip_bound = math.sqrt(features * outs)
    return call(
        functools.partial(combine_kernel, clip_bound),
        jax.ShapeDtypeStruct((LANE, outs // DP), F32),
        [whole()] * (DP + 1),
        whole(),
        scalars=1,
    )(dp[None], squares, *arrived)


def solution(mesh):
    fine = Mesh(mesh.devices.reshape(DP, X, Z, CORE), ("dp", "x", "z", "core"))
    ctx = ("x", "z", "core")
    in_specs = (P("dp", ctx, None), P(), P("dp", ctx, None), P("dp"))
    out_specs = P(ctx, "dp")
    return jax.shard_map(
        per_device, mesh=fine, in_specs=in_specs, out_specs=out_specs, check_vma=False
    )
```

```python
import functools
import math

import jax
import jax.numpy as jnp
from jax import lax
from jax.experimental import pallas as pl
from jax.experimental.pallas import tpu as pltpu
from jax.sharding import Mesh
from jax.sharding import PartitionSpec as P


X, Z, CORE, DP = 4, 8, 2, 4
LANE = 128
WIRE = jnp.bfloat16
VMEM = pltpu.VMEM
F32 = jnp.float32
HALVES = 2
PIECES = 4


def call(kernel, out_shape, in_specs, out_specs, scalars=0, scratch=(), flops=0, moved=0, mib=12):
    return pl.pallas_call(
        kernel,
        out_shape=out_shape,
        compiler_params=pltpu.CompilerParams(vmem_limit_bytes=mib << 20),
        grid_spec=pltpu.PrefetchScalarGridSpec(
            num_scalar_prefetch=scalars,
            grid=(),
            in_specs=in_specs,
            out_specs=out_specs,
            scratch_shapes=list(scratch),
        ),
        cost_estimate=pl.CostEstimate(flops=flops, bytes_accessed=moved, transcendentals=0),
    )


def whole():
    return pl.BlockSpec(memory_space=VMEM)


def prep_kernel(half, at_ref, hidden_ref, gain_ref, own_ref, send_ref):
    rows = own_ref.shape[0] // PIECES
    features = hidden_ref.shape[1]
    tiles = features // LANE
    core = at_ref[2]
    for n in range(PIECES):
        at = slice((half * PIECES + n) * rows, (half * PIECES + n + 1) * rows)
        total = jnp.zeros((rows, LANE), F32)
        for i in range(tiles):
            v = hidden_ref[at, i * LANE : (i + 1) * LANE].astype(F32)
            total = total + v * v
        mean = jnp.sum(total, axis=1, keepdims=True) * (1.0 / features)
        scale = jnp.broadcast_to(lax.rsqrt(mean + 1e-05), (rows, LANE))
        for out, parity in ((send_ref, 1 - core), (own_ref, core)):
            for i in range(tiles // 2):
                tile = 2 * i + parity
                v = hidden_ref[at, pl.ds(pl.multiple_of(tile * LANE, LANE), LANE)].astype(F32)
                v = v * scale * gain_ref[pl.ds(tile, 1), :]
                out[n * rows : (n + 1) * rows, i * LANE : (i + 1) * LANE] = v.astype(out.dtype)


def prep(half, hidden, gain, at):
    tokens, features = hidden.shape
    rows = tokens // HALVES
    part = jax.ShapeDtypeStruct((rows, features // 2), jnp.bfloat16)
    return call(
        functools.partial(prep_kernel, half),
        (part, part),
        [whole(), whole()],
        (whole(), whole()),
        scalars=1,
        flops=4 * rows * features,
        moved=4 * rows * features,
        mib=14,
    )(at, hidden, gain)


def product_kernel(turns, at_ref, *refs):
    owner = jnp.bitwise_and(at_ref[0] + turns, X - 1)
    tokens = refs[: 2 * HALVES]
    cot_refs = refs[2 * HALVES : 2 * HALVES + 2]
    outs = refs[2 * HALVES + 2 :]
    half = cot_refs[0].shape[0] // 2
    rows = tokens[0].shape[0]
    for p in range(Z // 2):
        lanes = pl.ds(pl.multiple_of(owner * (Z * LANE) + p * 2 * LANE, 2 * LANE), 2 * LANE)
        total = None
        for n, t in enumerate(tokens):
            c = cot_refs[n // HALVES][:, (n % HALVES) * rows : (n % HALVES + 1) * rows]
            term = jnp.dot(c, t[:, lanes], preferred_element_type=F32)
            total = term if total is None else total + term
        for i in range(2):
            at = slice((2 * p + i) * half, (2 * p + i + 1) * half)
            tile = total[:, i * LANE : (i + 1) * LANE]
            outs[0][at, :] = tile[:half].astype(outs[0].dtype)
            outs[1][at, :] = tile[half:].astype(outs[1].dtype)


def product(turns, own, par, cto, ctp, at):
    outs = cto.shape[0]
    tokens = 2 * cto.shape[1]
    shape = jax.ShapeDtypeStruct((Z * outs // 2, LANE), WIRE if turns else F32)
    return call(
        functools.partial(product_kernel, turns),
        (shape, shape),
        [whole()] * (2 * HALVES + 2),
        (whole(), whole()),
        scalars=1,
        flops=2 * outs * tokens * Z * LANE,
        moved=4 * tokens * Z * LANE,
        mib=14,
    )(at, *own, *par, cto, ctp)


def gather_kernel(at_ref, own_ref, r1_ref, r2_ref, r3_ref, out_ref, mine_ref):
    half = own_ref.shape[0] // Z

    def total(at):
        value = own_ref[at, :]
        for r in (r1_ref, r2_ref, r3_ref):
            value = value + r[at, :].astype(F32)
        return value

    for j in range(Z):
        out_ref[j] = total(slice(j * half, (j + 1) * half)).astype(out_ref.dtype)
    mine_ref[...] = total(pl.ds(pl.multiple_of(at_ref[1] * half, half), half))


def gather(own, r1, r2, r3, at):
    half = own.shape[0] // Z
    return call(
        gather_kernel,
        (jax.ShapeDtypeStruct((Z, half, LANE), WIRE), jax.ShapeDtypeStruct((half, LANE), F32)),
        [whole()] * 4,
        (whole(), whole()),
        scalars=1,
        flops=4 * own.size,
        moved=12 * own.size,
    )(at, own, r1, r2, r3)


def finish_kernel(at_ref, weight_ref, *refs):
    mine, arrived, outs = refs[:2], refs[2:4], refs[4 : 4 + DP]
    squares_ref, tile = refs[4 + DP :]
    half = mine[0].shape[0]
    weight = weight_ref[0]
    squares = jnp.zeros((1, LANE), F32)
    for n in range(2):
        total = mine[n][...]
        for j in range(Z):
            other = jnp.where(at_ref[1] == j, 0.0, 1.0)
            total = total + arrived[n][j].astype(F32) * other
        total = total * weight
        tile[n * half : (n + 1) * half, :] = total
        squares = squares + jnp.sum(total * total, axis=0, keepdims=True)
    rows = 2 * half // DP
    for k in range(DP):
        owner = jnp.bitwise_and(at_ref[3] + k, DP - 1)
        outs[k][...] = tile[pl.ds(pl.multiple_of(owner * rows, rows), rows), :]
    squares_ref[...] = jnp.broadcast_to(squares[None], squares_ref.shape)


def finish(mine, arrived, at, weight):
    half = mine[0].shape[0]
    block = jax.ShapeDtypeStruct((2 * half // DP, LANE), F32)
    return call(
        finish_kernel,
        (block,) * DP + (jax.ShapeDtypeStruct((Z * CORE, 1, LANE), F32),),
        [pl.BlockSpec(memory_space=pltpu.SMEM)] + [whole()] * 4,
        (whole(),) * (DP + 1),
        scalars=1,
        scratch=[VMEM((2 * half, LANE), F32)],
        flops=4 * arrived[0].size,
        moved=4 * arrived[0].size,
    )(at, weight, *mine, *arrived)


def pass_kernel(in_ref, out_ref):
    out_ref[...] = jnp.broadcast_to(jnp.sum(in_ref[...], axis=0, keepdims=True), out_ref.shape)


def keep_kernel(in_ref, out_ref):
    out_ref[...] = in_ref[...]


def keep(value):
    return call(keep_kernel, jax.ShapeDtypeStruct(value.shape, value.dtype), [whole()], whole())(value)


def combine_kernel(clip_bound, at_ref, squares_ref, *refs):
    blocks, out_ref = refs[:DP], refs[DP]
    total = None
    for k in range(DP):
        example = jnp.bitwise_and(at_ref[3] + DP - k, DP - 1)
        squares = jnp.sum(squares_ref[pl.ds(example * X, X)])
        factor = jnp.minimum(1.0, clip_bound * lax.rsqrt(jnp.full((1, LANE), squares, F32) + 1e-06))
        term = blocks[k][...] * factor
        total = term if total is None else total + term
    out_ref[...] = total.T


def turn(n, k):
    return [(i, (i + k) % n) for i in range(n)]


def exchanged(value, axis):
    return lax.all_to_all(value, axis, split_axis=0, concat_axis=0, tiled=True)


def per_device(hidden, norm_gain, cotangent, loss_weight):
    hidden, cot = hidden[0], cotangent[0]
    tokens, features = hidden.shape
    outs = cot.shape[1]
    doc_length = tokens * X * Z * CORE
    at = jnp.stack([lax.axis_index(n).astype(jnp.int32) for n in ("x", "z", "core", "dp")])
    swap = functools.partial(lax.ppermute, axis_name="core", perm=turn(CORE, 1))
    gain = norm_gain.reshape(features // LANE, LANE)
    weight = loss_weight * (1.0 / math.sqrt(doc_length))
    hidden, gain, weight, at, cto = lax.optimization_barrier((hidden, gain, weight, at, cot.T))
    ctp = swap(cto)
    own, par = [], []
    for half in range(HALVES):
        kept, sent = prep(half, hidden, gain, at)
        own.append(kept)
        par.append(swap(sent))

    def block(k):
        return product(k, own, par, cto, ctp, at)

    blocks = {k: block(k) for k in (2, 1, 3, 0)}
    mine, summed = [], []
    for chunk in range(2):
        arrived = [lax.ppermute(blocks[k][chunk], "x", turn(X, k)) for k in (2, 1, 3)]
        ready, kept = gather(blocks[0][chunk], *arrived, at)
        mine.append(kept)
        summed.append(exchanged(ready, "z"))
    *tiles, squares = finish(mine, summed, at, weight)
    arrived = [tiles[0]] + [lax.ppermute(tiles[k], "dp", turn(DP, k)) for k in range(1, DP)]
    arrived[0] = keep(arrived[0])
    squares = exchanged(squares, ("z", "core"))
    squares = call(pass_kernel, jax.ShapeDtypeStruct((DP * X, 1, LANE), F32), [whole()], whole())(squares)
    squares = exchanged(squares, ("dp", "x"))
    clip_bound = math.sqrt(features * outs)
    return call(
        functools.partial(combine_kernel, clip_bound),
        jax.ShapeDtypeStruct((LANE, outs // DP), F32),
        [whole()] * (DP + 1),
        whole(),
        scalars=1,
    )(at, squares, *arrived)


def solution(mesh):
    fine = Mesh(mesh.devices.reshape(DP, X, Z, CORE), ("dp", "x", "z", "core"))
    ctx = ("x", "z", "core")
    in_specs = (P("dp", ctx, None), P(), P("dp", ctx, None), P("dp"))
    out_specs = P(ctx, "dp")
    return jax.shard_map(
        per_device, mesh=fine, in_specs=in_specs, out_specs=out_specs, check_vma=False
    )
```

```python
import functools
import math

import jax
import jax.numpy as jnp
from jax import lax
from jax.experimental import pallas as pl
from jax.experimental.pallas import tpu as pltpu
from jax.sharding import Mesh
from jax.sharding import PartitionSpec as P


X, Z, CORE, DP = 4, 8, 2, 4
LANE = 128
WIRE = jnp.bfloat16
VMEM = pltpu.VMEM
F32 = jnp.float32
HALVES = 2
PIECES = 4


def call(kernel, out_shape, in_specs, out_specs, scalars=0, scratch=(), flops=0, moved=0, mib=12):
    return pl.pallas_call(
        kernel,
        out_shape=out_shape,
        compiler_params=pltpu.CompilerParams(vmem_limit_bytes=mib << 20),
        grid_spec=pltpu.PrefetchScalarGridSpec(
            num_scalar_prefetch=scalars,
            grid=(),
            in_specs=in_specs,
            out_specs=out_specs,
            scratch_shapes=list(scratch),
        ),
        cost_estimate=pl.CostEstimate(flops=flops, bytes_accessed=moved, transcendentals=0),
    )


def whole():
    return pl.BlockSpec(memory_space=VMEM)


def prep_kernel(half, at_ref, hidden_ref, gain_ref, own_ref, send_ref):
    rows = own_ref.shape[0] // PIECES
    features = hidden_ref.shape[1]
    tiles = features // LANE
    core = at_ref[2]
    for n in range(PIECES):
        at = slice((half * PIECES + n) * rows, (half * PIECES + n + 1) * rows)
        total = jnp.zeros((rows, LANE), F32)
        for i in range(tiles):
            v = hidden_ref[at, i * LANE : (i + 1) * LANE].astype(F32)
            total = total + v * v
        mean = jnp.sum(total, axis=1, keepdims=True) * (1.0 / features)
        scale = jnp.broadcast_to(lax.rsqrt(mean + 1e-05), (rows, LANE))
        for out, parity in ((send_ref, 1 - core), (own_ref, core)):
            for i in range(tiles // 2):
                tile = 2 * i + parity
                v = hidden_ref[at, pl.ds(pl.multiple_of(tile * LANE, LANE), LANE)].astype(F32)
                v = v * scale * gain_ref[pl.ds(tile, 1), :]
                out[n * rows : (n + 1) * rows, i * LANE : (i + 1) * LANE] = v.astype(out.dtype)


def prep(half, hidden, gain, at):
    tokens, features = hidden.shape
    rows = tokens // HALVES
    part = jax.ShapeDtypeStruct((rows, features // 2), jnp.bfloat16)
    return call(
        functools.partial(prep_kernel, half),
        (part, part),
        [whole(), whole()],
        (whole(), whole()),
        scalars=1,
        flops=4 * rows * features,
        moved=4 * rows * features,
        mib=14,
    )(at, hidden, gain)


def turn_kernel(in_ref, out_ref):
    out_ref[...] = in_ref[...].T


def turned(value):
    return call(turn_kernel, jax.ShapeDtypeStruct(value.shape[::-1], value.dtype), [whole()], whole())(value)


def product_kernel(turns, chunk, at_ref, *refs):
    owner = jnp.bitwise_and(at_ref[0] + turns, X - 1)
    tokens = refs[: 2 * HALVES]
    cot_refs = refs[2 * HALVES : 2 * HALVES + 2]
    out_ref = refs[2 * HALVES + 2]
    half = cot_refs[0].shape[0] // 2
    rows = tokens[0].shape[0]
    for p in range(Z // 2):
        lanes = pl.ds(pl.multiple_of(owner * (Z * LANE) + p * 2 * LANE, 2 * LANE), 2 * LANE)
        total = None
        for n, t in enumerate(tokens):
            c = cot_refs[n // HALVES]
            c = c[chunk * half : (chunk + 1) * half, (n % HALVES) * rows : (n % HALVES + 1) * rows]
            term = jnp.dot(c, t[:, lanes], preferred_element_type=F32)
            total = term if total is None else total + term
        for i in range(2):
            at = slice((2 * p + i) * half, (2 * p + i + 1) * half)
            out_ref[at, :] = total[:, i * LANE : (i + 1) * LANE].astype(out_ref.dtype)


def product(turns, chunk, own, par, cto, ctp, at):
    outs = cto.shape[0] // 2
    tokens = 2 * cto.shape[1]
    return call(
        functools.partial(product_kernel, turns, chunk),
        jax.ShapeDtypeStruct((Z * outs, LANE), WIRE if turns else F32),
        [whole()] * (2 * HALVES + 2),
        whole(),
        scalars=1,
        flops=2 * outs * tokens * Z * LANE,
        moved=4 * tokens * Z * LANE,
        mib=14,
    )(at, *own, *par, cto, ctp)


def gather_kernel(at_ref, own_ref, r1_ref, r2_ref, r3_ref, out_ref, mine_ref):
    half = own_ref.shape[0] // Z

    def total(at):
        value = own_ref[at, :]
        for r in (r1_ref, r2_ref, r3_ref):
            value = value + r[at, :].astype(F32)
        return value

    for j in range(Z):
        out_ref[j] = total(slice(j * half, (j + 1) * half)).astype(out_ref.dtype)
    mine_ref[...] = total(pl.ds(pl.multiple_of(at_ref[1] * half, half), half))


def gather(own, r1, r2, r3, at):
    half = own.shape[0] // Z
    return call(
        gather_kernel,
        (jax.ShapeDtypeStruct((Z, half, LANE), WIRE), jax.ShapeDtypeStruct((half, LANE), F32)),
        [whole()] * 4,
        (whole(), whole()),
        scalars=1,
        flops=4 * own.size,
        moved=12 * own.size,
    )(at, own, r1, r2, r3)


def finished(at_ref, weight_ref, mine_ref, arrived_ref):
    total = mine_ref[...]
    for j in range(Z):
        total = total + arrived_ref[j].astype(F32) * jnp.where(at_ref[1] == j, 0.0, 1.0)
    total = total * weight_ref[0]
    return total, jnp.sum(total * total, axis=0, keepdims=True)


def first_kernel(at_ref, weight_ref, mine_ref, arrived_ref, tile_ref, squares_ref):
    total, squares = finished(at_ref, weight_ref, mine_ref, arrived_ref)
    tile_ref[...] = total
    squares_ref[...] = jnp.broadcast_to(squares, squares_ref.shape)


def first(mine, arrived, at, weight):
    return call(
        first_kernel,
        (jax.ShapeDtypeStruct(mine.shape, F32), jax.ShapeDtypeStruct((8, LANE), F32)),
        [pl.BlockSpec(memory_space=pltpu.SMEM)] + [whole()] * 2,
        (whole(), whole()),
        scalars=1,
        flops=4 * arrived.size,
        moved=4 * arrived.size,
    )(at, weight, mine, arrived)


def last_kernel(at_ref, weight_ref, mine_ref, arrived_ref, before_ref, partial_ref, *refs):
    outs, squares_ref, tile = refs[:DP], refs[DP], refs[DP + 1]
    total, squares = finished(at_ref, weight_ref, mine_ref, arrived_ref)
    half = total.shape[0]
    squares_ref[...] = jnp.broadcast_to((squares + partial_ref[:1, :])[None], squares_ref.shape)
    tile[:half, :] = before_ref[...]
    tile[half:, :] = total
    rows = 2 * half // DP
    for k in range(DP):
        owner = jnp.bitwise_and(at_ref[3] + k, DP - 1)
        outs[k][...] = tile[pl.ds(pl.multiple_of(owner * rows, rows), rows), :]


def last(mine, arrived, before, partial, at, weight):
    half = mine.shape[0]
    block = jax.ShapeDtypeStruct((2 * half // DP, LANE), F32)
    return call(
        last_kernel,
        (block,) * DP + (jax.ShapeDtypeStruct((Z * CORE, 1, LANE), F32),),
        [pl.BlockSpec(memory_space=pltpu.SMEM)] + [whole()] * 4,
        (whole(),) * (DP + 1),
        scalars=1,
        scratch=[VMEM((2 * half, LANE), F32)],
        flops=4 * arrived.size,
        moved=4 * arrived.size,
    )(at, weight, mine, arrived, before, partial)


def pass_kernel(in_ref, out_ref):
    out_ref[...] = jnp.broadcast_to(jnp.sum(in_ref[...], axis=0, keepdims=True), out_ref.shape)


def keep_kernel(in_ref, out_ref):
    out_ref[...] = in_ref[...]


def keep(value):
    return call(keep_kernel, jax.ShapeDtypeStruct(value.shape, value.dtype), [whole()], whole())(value)


def upright_kernel(*refs):
    for n in range(DP):
        refs[DP][n] = refs[n][...].T


def combine_kernel(clip_bound, at_ref, squares_ref, blocks_ref, out_ref):
    total = None
    for k in range(DP):
        example = jnp.bitwise_and(at_ref[3] + DP - k, DP - 1)
        squares = jnp.sum(squares_ref[pl.ds(example * X, X)])
        factor = jnp.minimum(1.0, clip_bound * lax.rsqrt(jnp.full((1, LANE), squares, F32) + 1e-06))
        term = blocks_ref[k] * factor
        total = term if total is None else total + term
    out_ref[...] = total


def turn(n, k):
    return [(i, (i + k) % n) for i in range(n)]


def exchanged(value, axis):
    return lax.all_to_all(value, axis, split_axis=0, concat_axis=0, tiled=True)


def per_device(hidden, norm_gain, cotangent, loss_weight):
    hidden, cot = hidden[0], cotangent[0]
    tokens, features = hidden.shape
    outs = cot.shape[1]
    doc_length = tokens * X * Z * CORE
    at = jnp.stack([lax.axis_index(n).astype(jnp.int32) for n in ("x", "z", "core", "dp")])
    swap = functools.partial(lax.ppermute, axis_name="core", perm=turn(CORE, 1))
    gain = norm_gain.reshape(features // LANE, LANE)
    weight = loss_weight * (1.0 / math.sqrt(doc_length))
    hidden, gain, weight, at = lax.optimization_barrier((hidden, gain, weight, at))
    own, par = [], []
    for half in range(HALVES):
        kept, sent = prep(half, hidden, gain, at)
        own.append(kept)
        par.append(swap(sent))

    cto = turned(cot)
    ctp = swap(cto)

    def block(k, chunk):
        return product(k, chunk, own, par, cto, ctp, at)

    order = [(k, chunk) for chunk in range(2) for k in (2, 1, 3)] + [(0, 0), (0, 1)]
    blocks = {n: block(*n) for n in order}
    mine, summed = [], []
    for chunk in range(2):
        arrived = []
        for k in (2, 1, 3):
            arrived.append(lax.ppermute(blocks[k, chunk], "x", turn(X, k)))
        ready, kept = gather(blocks[0, chunk], *arrived, at)
        mine.append(kept)
        summed.append(exchanged(ready, "z"))
    before, partial = first(mine[0], summed[0], at, weight)
    *tiles, squares = last(mine[1], summed[1], before, partial, at, weight)
    arrived = [lax.ppermute(tiles[k], "dp", turn(DP, k)) for k in range(1, DP)]
    kept = keep(tiles[0])
    squares = exchanged(squares, ("z", "core"))
    squares = call(pass_kernel, jax.ShapeDtypeStruct((DP * X, 1, LANE), F32), [whole()], whole())(squares)
    shape = jax.ShapeDtypeStruct((DP, LANE, outs // DP), F32)
    blocks = call(upright_kernel, shape, [whole()] * DP, whole())(kept, *arrived)
    squares = exchanged(squares, ("dp", "x"))
    clip_bound = math.sqrt(features * outs)
    return call(
        functools.partial(combine_kernel, clip_bound),
        jax.ShapeDtypeStruct((LANE, outs // DP), F32),
        [whole()] * 2,
        whole(),
        scalars=1,
    )(at, squares, blocks)


def solution(mesh):
    fine = Mesh(mesh.devices.reshape(DP, X, Z, CORE), ("dp", "x", "z", "core"))
    ctx = ("x", "z", "core")
    in_specs = (P("dp", ctx, None), P(), P("dp", ctx, None), P("dp"))
    out_specs = P(ctx, "dp")
    return jax.shard_map(
        per_device, mesh=fine, in_specs=in_specs, out_specs=out_specs, check_vma=False
    )
```

```python
import functools
import math

import jax
import jax.numpy as jnp
from jax import lax
from jax.experimental import pallas as pl
from jax.experimental.pallas import tpu as pltpu
from jax.sharding import Mesh
from jax.sharding import PartitionSpec as P


X, Z, CORE, DP = 4, 8, 2, 4
LANE = 128
WIRE = jnp.bfloat16
VMEM = pltpu.VMEM
F32 = jnp.float32
HALVES = 2
PIECES = 4
CUTS = (0, 192, 384, 512)
CHUNKS = range(len(CUTS) - 1)


def call(kernel, out_shape, in_specs, out_specs, scalars=0, scratch=(), flops=0, moved=0, mib=12):
    return pl.pallas_call(
        kernel,
        out_shape=out_shape,
        compiler_params=pltpu.CompilerParams(vmem_limit_bytes=mib << 20),
        grid_spec=pltpu.PrefetchScalarGridSpec(
            num_scalar_prefetch=scalars,
            grid=(),
            in_specs=in_specs,
            out_specs=out_specs,
            scratch_shapes=list(scratch),
        ),
        cost_estimate=pl.CostEstimate(flops=flops, bytes_accessed=moved, transcendentals=0),
    )


def whole():
    return pl.BlockSpec(memory_space=VMEM)


def prep_kernel(half, at_ref, hidden_ref, gain_ref, own_ref, send_ref):
    rows = own_ref.shape[0] // PIECES
    features = hidden_ref.shape[1]
    tiles = features // LANE
    core = at_ref[2]
    for n in range(PIECES):
        at = slice((half * PIECES + n) * rows, (half * PIECES + n + 1) * rows)
        total = jnp.zeros((rows, LANE), F32)
        for i in range(tiles):
            v = hidden_ref[at, i * LANE : (i + 1) * LANE].astype(F32)
            total = total + v * v
        mean = jnp.sum(total, axis=1, keepdims=True) * (1.0 / features)
        scale = jnp.broadcast_to(lax.rsqrt(mean + 1e-05), (rows, LANE))
        for out, parity in ((send_ref, 1 - core), (own_ref, core)):
            for i in range(tiles // 2):
                tile = 2 * i + parity
                v = hidden_ref[at, pl.ds(pl.multiple_of(tile * LANE, LANE), LANE)].astype(F32)
                v = v * scale * gain_ref[pl.ds(tile, 1), :]
                out[n * rows : (n + 1) * rows, i * LANE : (i + 1) * LANE] = v.astype(out.dtype)


def prep(half, hidden, gain, at):
    tokens, features = hidden.shape
    rows = tokens // HALVES
    part = jax.ShapeDtypeStruct((rows, features // 2), jnp.bfloat16)
    return call(
        functools.partial(prep_kernel, half),
        (part, part),
        [whole(), whole()],
        (whole(), whole()),
        scalars=1,
        flops=4 * rows * features,
        moved=4 * rows * features,
        mib=14,
    )(at, hidden, gain)


def turn_kernel(in_ref, out_ref):
    out_ref[...] = in_ref[...].T


def turned(value):
    return call(turn_kernel, jax.ShapeDtypeStruct(value.shape[::-1], value.dtype), [whole()], whole())(value)


def product_kernel(turns, chunk, at_ref, *refs):
    owner = jnp.bitwise_and(at_ref[0] + turns, X - 1)
    tokens = refs[: 2 * HALVES]
    cot_refs = refs[2 * HALVES : 2 * HALVES + 2]
    out_ref = refs[2 * HALVES + 2]
    cut = slice(CUTS[chunk], CUTS[chunk + 1])
    half = CUTS[chunk + 1] - CUTS[chunk]
    rows = tokens[0].shape[0]
    for p in range(Z // 2):
        lanes = pl.ds(pl.multiple_of(owner * (Z * LANE) + p * 2 * LANE, 2 * LANE), 2 * LANE)
        total = None
        for n, t in enumerate(tokens):
            c = cot_refs[n // HALVES]
            c = c[cut, (n % HALVES) * rows : (n % HALVES + 1) * rows]
            term = jnp.dot(c, t[:, lanes], preferred_element_type=F32)
            total = term if total is None else total + term
        for i in range(2):
            at = slice((2 * p + i) * half, (2 * p + i + 1) * half)
            out_ref[at, :] = total[:, i * LANE : (i + 1) * LANE].astype(out_ref.dtype)


def product(turns, chunk, own, par, cto, ctp, at):
    outs = CUTS[chunk + 1] - CUTS[chunk]
    tokens = 2 * cto.shape[1]
    return call(
        functools.partial(product_kernel, turns, chunk),
        jax.ShapeDtypeStruct((Z * outs, LANE), WIRE if turns else F32),
        [whole()] * (2 * HALVES + 2),
        whole(),
        scalars=1,
        flops=2 * outs * tokens * Z * LANE,
        moved=4 * tokens * Z * LANE,
        mib=14,
    )(at, *own, *par, cto, ctp)


def gather_kernel(at_ref, own_ref, r1_ref, r2_ref, r3_ref, out_ref, mine_ref):
    half = own_ref.shape[0] // Z

    def total(at):
        value = own_ref[at, :]
        for r in (r1_ref, r2_ref, r3_ref):
            value = value + r[at, :].astype(F32)
        return value

    for j in range(Z):
        out_ref[j] = total(slice(j * half, (j + 1) * half)).astype(out_ref.dtype)
    mine_ref[...] = total(pl.ds(pl.multiple_of(at_ref[1] * half, half), half))


def gather(own, r1, r2, r3, at):
    half = own.shape[0] // Z
    return call(
        gather_kernel,
        (jax.ShapeDtypeStruct((Z, half, LANE), WIRE), jax.ShapeDtypeStruct((half, LANE), F32)),
        [whole()] * 4,
        (whole(), whole()),
        scalars=1,
        flops=4 * own.size,
        moved=12 * own.size,
    )(at, own, r1, r2, r3)


def finished(at_ref, weight_ref, mine_ref, arrived_ref):
    total = mine_ref[...]
    for j in range(Z):
        total = total + arrived_ref[j].astype(F32) * jnp.where(at_ref[1] == j, 0.0, 1.0)
    total = total * weight_ref[0]
    return total, jnp.sum(total * total, axis=0, keepdims=True)


def first_kernel(at_ref, weight_ref, mine_ref, arrived_ref, tile_ref, squares_ref):
    total, squares = finished(at_ref, weight_ref, mine_ref, arrived_ref)
    tile_ref[...] = total
    squares_ref[...] = jnp.broadcast_to(squares, squares_ref.shape)


def first(mine, arrived, at, weight):
    return call(
        first_kernel,
        (jax.ShapeDtypeStruct(mine.shape, F32), jax.ShapeDtypeStruct((8, LANE), F32)),
        [pl.BlockSpec(memory_space=pltpu.SMEM)] + [whole()] * 2,
        (whole(), whole()),
        scalars=1,
        flops=4 * arrived.size,
        moved=4 * arrived.size,
    )(at, weight, mine, arrived)


def last_kernel(at_ref, weight_ref, mine_ref, arrived_ref, *refs):
    before = refs[: 2 * len(CHUNKS) - 2]
    outs, squares_ref, tile = refs[len(before) : len(before) + DP], refs[-2], refs[-1]
    total, squares = finished(at_ref, weight_ref, mine_ref, arrived_ref)
    for n in CHUNKS[:-1]:
        tile[CUTS[n] : CUTS[n + 1], :] = before[2 * n][...]
        squares = squares + before[2 * n + 1][:1, :]
    squares_ref[...] = jnp.broadcast_to(squares[None], squares_ref.shape)
    tile[CUTS[-2] :, :] = total
    rows = CUTS[-1] // DP
    for k in range(DP):
        owner = jnp.bitwise_and(at_ref[3] + k, DP - 1)
        outs[k][...] = tile[pl.ds(pl.multiple_of(owner * rows, rows), rows), :]


def last(mine, arrived, before, at, weight):
    block = jax.ShapeDtypeStruct((CUTS[-1] // DP, LANE), F32)
    return call(
        last_kernel,
        (block,) * DP + (jax.ShapeDtypeStruct((Z * CORE, 1, LANE), F32),),
        [pl.BlockSpec(memory_space=pltpu.SMEM)] + [whole()] * (2 + len(before)),
        (whole(),) * (DP + 1),
        scalars=1,
        scratch=[VMEM((CUTS[-1], LANE), F32)],
        flops=4 * arrived.size,
        moved=4 * arrived.size,
    )(at, weight, mine, arrived, *before)


def pass_kernel(in_ref, out_ref):
    out_ref[...] = jnp.broadcast_to(jnp.sum(in_ref[...], axis=0, keepdims=True), out_ref.shape)


def keep_kernel(in_ref, out_ref):
    out_ref[...] = in_ref[...]


def keep(value):
    return call(keep_kernel, jax.ShapeDtypeStruct(value.shape, value.dtype), [whole()], whole())(value)


def upright_kernel(*refs):
    for n in range(DP):
        refs[DP][n] = refs[n][...].T


def combine_kernel(clip_bound, at_ref, squares_ref, blocks_ref, out_ref):
    total = None
    for k in range(DP):
        example = jnp.bitwise_and(at_ref[3] + DP - k, DP - 1)
        squares = jnp.sum(jnp.sum(squares_ref[pl.ds(example * X, X)], axis=0), axis=1, keepdims=True)
        factor = jnp.minimum(1.0, clip_bound * lax.rsqrt(squares + 1e-06))
        term = blocks_ref[k] * factor
        total = term if total is None else total + term
    out_ref[...] = total


def turn(n, k):
    return [(i, (i + k) % n) for i in range(n)]


def exchanged(value, axis):
    return lax.all_to_all(value, axis, split_axis=0, concat_axis=0, tiled=True)


def per_device(hidden, norm_gain, cotangent, loss_weight):
    hidden, cot = hidden[0], cotangent[0]
    tokens, features = hidden.shape
    outs = cot.shape[1]
    doc_length = tokens * X * Z * CORE
    at = jnp.stack([lax.axis_index(n).astype(jnp.int32) for n in ("x", "z", "core", "dp")])
    swap = functools.partial(lax.ppermute, axis_name="core", perm=turn(CORE, 1))
    gain = norm_gain.reshape(features // LANE, LANE)
    weight = loss_weight * (1.0 / math.sqrt(doc_length))
    hidden, gain, weight, at = lax.optimization_barrier((hidden, gain, weight, at))
    own, par = [], []
    for half in range(HALVES):
        kept, sent = prep(half, hidden, gain, at)
        own.append(kept)
        par.append(swap(sent))

    cto = turned(cot)
    ctp = swap(cto)

    def block(k, chunk):
        return product(k, chunk, own, par, cto, ctp, at)

    order = [(k, chunk) for chunk in CHUNKS for k in (2, 1, 3)] + [(0, chunk) for chunk in CHUNKS]
    blocks = {n: block(*n) for n in order}
    mine, summed = [], []
    for chunk in CHUNKS:
        arrived = []
        for k in (2, 1, 3):
            arrived.append(lax.ppermute(blocks[k, chunk], "x", turn(X, k)))
        ready, kept = gather(blocks[0, chunk], *arrived, at)
        mine.append(kept)
        summed.append(exchanged(ready, "z"))
    before = []
    for n in CHUNKS[:-1]:
        before += first(mine[n], summed[n], at, weight)
    *tiles, squares = last(mine[-1], summed[-1], before, at, weight)
    arrived = [lax.ppermute(tiles[k], "dp", turn(DP, k)) for k in range(1, DP)]
    kept = keep(tiles[0])
    squares = exchanged(squares, ("z", "core"))
    squares = call(pass_kernel, jax.ShapeDtypeStruct((DP * X, 1, LANE), F32), [whole()], whole())(squares)
    shape = jax.ShapeDtypeStruct((DP, LANE, outs // DP), F32)
    blocks = call(upright_kernel, shape, [whole()] * DP, whole())(kept, *arrived)
    squares = exchanged(squares, ("dp", "x"))
    clip_bound = math.sqrt(features * outs)
    return call(
        functools.partial(combine_kernel, clip_bound),
        jax.ShapeDtypeStruct((LANE, outs // DP), F32),
        [whole()] * 2,
        whole(),
        scalars=1,
    )(at, squares, blocks)


def solution(mesh):
    fine = Mesh(mesh.devices.reshape(DP, X, Z, CORE), ("dp", "x", "z", "core"))
    ctx = ("x", "z", "core")
    in_specs = (P("dp", ctx, None), P(), P("dp", ctx, None), P("dp"))
    out_specs = P(ctx, "dp")
    return jax.shard_map(
        per_device, mesh=fine, in_specs=in_specs, out_specs=out_specs, check_vma=False
    )
```

```python
import functools
import math

import jax
import jax.numpy as jnp
from jax import lax
from jax.experimental import pallas as pl
from jax.experimental.pallas import tpu as pltpu
from jax.sharding import Mesh
from jax.sharding import PartitionSpec as P


X, Z, CORE, DP = 4, 8, 2, 4
LANE = 128
WIRE = jnp.bfloat16
VMEM = pltpu.VMEM
F32 = jnp.float32
PIECES = 8
CUTS = (0, 256, 512)
CHUNKS = range(len(CUTS) - 1)


def call(kernel, out_shape, in_specs, out_specs, scalars=0, scratch=(), flops=0, moved=0, mib=12):
    return pl.pallas_call(
        kernel,
        out_shape=out_shape,
        compiler_params=pltpu.CompilerParams(vmem_limit_bytes=mib << 20),
        grid_spec=pltpu.PrefetchScalarGridSpec(
            num_scalar_prefetch=scalars,
            grid=(),
            in_specs=in_specs,
            out_specs=out_specs,
            scratch_shapes=list(scratch),
        ),
        cost_estimate=pl.CostEstimate(flops=flops, bytes_accessed=moved, transcendentals=0),
    )


def whole():
    return pl.BlockSpec(memory_space=VMEM)


def pieces_into(pieces, at_ref, hidden_ref, gain_ref, scale_ref, outs):
    tokens = hidden_ref.shape[0]
    rows = tokens // PIECES
    for n in range(PIECES):
        at = slice(n * rows, (n + 1) * rows)
        scale = scale_ref[at, :]
        for (turns, side), out in zip(pieces, outs):
            owner = jnp.bitwise_and(at_ref[0] + turns, X - 1)
            parity = at_ref[2] if side == 0 else 1 - at_ref[2]
            for i in range(Z):
                tile = owner * (2 * Z) + 2 * i + parity
                v = hidden_ref[at, pl.ds(pl.multiple_of(tile * LANE, LANE), LANE)].astype(F32)
                v = v * scale * gain_ref[pl.ds(tile, 1), :]
                out[at, i * LANE : (i + 1) * LANE] = v.astype(out.dtype)


def scale_kernel(pieces, at_ref, hidden_ref, gain_ref, scale_ref, *outs):
    tokens, features = hidden_ref.shape
    rows = tokens // PIECES
    for n in range(PIECES):
        at = slice(n * rows, (n + 1) * rows)
        total = jnp.zeros((rows, LANE), F32)
        for i in range(features // LANE):
            v = hidden_ref[at, i * LANE : (i + 1) * LANE].astype(F32)
            total = total + v * v
        mean = jnp.sum(total, axis=1, keepdims=True) * (1.0 / features)
        scale_ref[at, :] = jnp.broadcast_to(lax.rsqrt(mean + 1e-05), (rows, LANE))
    pieces_into(pieces, at_ref, hidden_ref, gain_ref, scale_ref, outs)


def pieces_kernel(pieces, at_ref, hidden_ref, gain_ref, scale_ref, *outs):
    pieces_into(pieces, at_ref, hidden_ref, gain_ref, scale_ref, outs)


def prep(pieces, hidden, gain, at, scale=None):
    tokens = hidden.shape[0]
    part = jax.ShapeDtypeStruct((tokens, Z * LANE), jnp.bfloat16)
    shapes = (part,) * len(pieces)
    kernel, given = pieces_kernel, (scale,)
    if scale is None:
        kernel, given = scale_kernel, ()
        shapes = (jax.ShapeDtypeStruct((tokens, LANE), F32), *shapes)
    return call(
        functools.partial(kernel, pieces),
        shapes,
        [whole()] * (2 + len(given)),
        (whole(),) * len(shapes),
        scalars=1,
        flops=4 * tokens * Z * LANE * len(pieces),
        moved=4 * tokens * Z * LANE * len(pieces),
        mib=16,
    )(at, hidden, gain, *given)


def turn_kernel(in_ref, out_ref):
    out_ref[...] = in_ref[...].T


def turned(value):
    return call(turn_kernel, jax.ShapeDtypeStruct(value.shape[::-1], value.dtype), [whole()], whole())(value)


def product_kernel(chunk, own_ref, par_ref, cto_ref, ctp_ref, out_ref):
    cut = slice(CUTS[chunk], CUTS[chunk + 1])
    half = CUTS[chunk + 1] - CUTS[chunk]
    for p in range(Z // 2):
        lanes = slice(p * 2 * LANE, (p + 1) * 2 * LANE)
        total = jnp.dot(cto_ref[cut, :], own_ref[:, lanes], preferred_element_type=F32)
        total = total + jnp.dot(ctp_ref[cut, :], par_ref[:, lanes], preferred_element_type=F32)
        for i in range(2):
            at = slice((2 * p + i) * half, (2 * p + i + 1) * half)
            out_ref[at, :] = total[:, i * LANE : (i + 1) * LANE].astype(out_ref.dtype)


def product(chunk, own, par, cto, ctp, dtype):
    outs = CUTS[chunk + 1] - CUTS[chunk]
    tokens = 2 * cto.shape[1]
    return call(
        functools.partial(product_kernel, chunk),
        jax.ShapeDtypeStruct((Z * outs, LANE), dtype),
        [whole()] * 4,
        whole(),
        flops=2 * outs * tokens * Z * LANE,
        moved=4 * tokens * Z * LANE,
        mib=14,
    )(own, par, cto, ctp)


def gather_kernel(at_ref, own_ref, r1_ref, r2_ref, r3_ref, out_ref, mine_ref):
    half = own_ref.shape[0] // Z

    def total(at):
        value = own_ref[at, :]
        for r in (r1_ref, r2_ref, r3_ref):
            value = value + r[at, :].astype(F32)
        return value

    for j in range(Z):
        out_ref[j] = total(slice(j * half, (j + 1) * half)).astype(out_ref.dtype)
    mine_ref[...] = total(pl.ds(pl.multiple_of(at_ref[1] * half, half), half))


def gather(own, r1, r2, r3, at):
    half = own.shape[0] // Z
    return call(
        gather_kernel,
        (jax.ShapeDtypeStruct((Z, half, LANE), WIRE), jax.ShapeDtypeStruct((half, LANE), F32)),
        [whole()] * 4,
        (whole(), whole()),
        scalars=1,
        flops=4 * own.size,
        moved=12 * own.size,
    )(at, own, r1, r2, r3)


def finished(at_ref, weight_ref, mine_ref, arrived_ref):
    total = mine_ref[...]
    for j in range(Z):
        total = total + arrived_ref[j].astype(F32) * jnp.where(at_ref[1] == j, 0.0, 1.0)
    total = total * weight_ref[0]
    return total, jnp.sum(total * total, axis=0, keepdims=True)


def first_kernel(at_ref, weight_ref, mine_ref, arrived_ref, tile_ref, squares_ref):
    total, squares = finished(at_ref, weight_ref, mine_ref, arrived_ref)
    tile_ref[...] = total
    squares_ref[...] = jnp.broadcast_to(squares, squares_ref.shape)


def first(mine, arrived, at, weight):
    return call(
        first_kernel,
        (jax.ShapeDtypeStruct(mine.shape, F32), jax.ShapeDtypeStruct((8, LANE), F32)),
        [pl.BlockSpec(memory_space=pltpu.SMEM)] + [whole()] * 2,
        (whole(), whole()),
        scalars=1,
        flops=4 * arrived.size,
        moved=4 * arrived.size,
    )(at, weight, mine, arrived)


def last_kernel(at_ref, weight_ref, mine_ref, arrived_ref, *refs):
    before = refs[: 2 * len(CHUNKS) - 2]
    outs, squares_ref, tile = refs[len(before) : len(before) + DP], refs[-2], refs[-1]
    total, squares = finished(at_ref, weight_ref, mine_ref, arrived_ref)
    for n in CHUNKS[:-1]:
        tile[CUTS[n] : CUTS[n + 1], :] = before[2 * n][...]
        squares = squares + before[2 * n + 1][:1, :]
    squares_ref[...] = jnp.broadcast_to(squares[None], squares_ref.shape)
    tile[CUTS[-2] :, :] = total
    rows = CUTS[-1] // DP
    for k in range(DP):
        owner = jnp.bitwise_and(at_ref[3] + k, DP - 1)
        outs[k][...] = tile[pl.ds(pl.multiple_of(owner * rows, rows), rows), :]


def last(mine, arrived, before, at, weight):
    block = jax.ShapeDtypeStruct((CUTS[-1] // DP, LANE), F32)
    return call(
        last_kernel,
        (block,) * DP + (jax.ShapeDtypeStruct((Z * CORE, 1, LANE), F32),),
        [pl.BlockSpec(memory_space=pltpu.SMEM)] + [whole()] * (2 + len(before)),
        (whole(),) * (DP + 1),
        scalars=1,
        scratch=[VMEM((CUTS[-1], LANE), F32)],
        flops=4 * arrived.size,
        moved=4 * arrived.size,
    )(at, weight, mine, arrived, *before)


def pass_kernel(in_ref, out_ref):
    out_ref[...] = jnp.broadcast_to(jnp.sum(in_ref[...], axis=0, keepdims=True), out_ref.shape)


def keep_kernel(in_ref, out_ref):
    out_ref[...] = in_ref[...]


def keep(value):
    return call(keep_kernel, jax.ShapeDtypeStruct(value.shape, value.dtype), [whole()], whole())(value)


def upright_kernel(*refs):
    for n in range(DP):
        refs[DP][n] = refs[n][...].T


def combine_kernel(clip_bound, at_ref, squares_ref, blocks_ref, out_ref):
    total = None
    for k in range(DP):
        example = jnp.bitwise_and(at_ref[3] + DP - k, DP - 1)
        squares = jnp.sum(jnp.sum(squares_ref[pl.ds(example * X, X)], axis=0), axis=1, keepdims=True)
        factor = jnp.minimum(1.0, clip_bound * lax.rsqrt(squares + 1e-06))
        term = blocks_ref[k] * factor
        total = term if total is None else total + term
    out_ref[...] = total


def turn(n, k):
    return [(i, (i + k) % n) for i in range(n)]


def exchanged(value, axis):
    return lax.all_to_all(value, axis, split_axis=0, concat_axis=0, tiled=True)


def per_device(hidden, norm_gain, cotangent, loss_weight):
    hidden, cot = hidden[0], cotangent[0]
    tokens, features = hidden.shape
    outs = cot.shape[1]
    doc_length = tokens * X * Z * CORE
    at = jnp.stack([lax.axis_index(n).astype(jnp.int32) for n in ("x", "z", "core", "dp")])
    swap = functools.partial(lax.ppermute, axis_name="core", perm=turn(CORE, 1))
    gain = norm_gain.reshape(features // LANE, LANE)
    weight = loss_weight * (1.0 / math.sqrt(doc_length))
    hidden, gain, weight, at = lax.optimization_barrier((hidden, gain, weight, at))
    own, par = {}, {}
    scale, sent = prep([(2, 1)], hidden, gain, at)
    par[2] = swap(sent)
    cto = turned(cot)
    ctp = swap(cto)
    sent = prep([(1, 1), (3, 1)], hidden, gain, at, scale)
    par[1], par[3] = swap(sent[0]), swap(sent[1])
    sent, own[2], own[1], own[3], own[0] = prep([(0, 1), (2, 0), (1, 0), (3, 0), (0, 0)], hidden, gain, at, scale)
    par[0] = swap(sent)

    def block(k, chunk):
        return product(chunk, own[k], par[k], cto, ctp, WIRE if k else F32)

    order = [(k, chunk) for chunk in CHUNKS for k in (2, 1, 3)] + [(0, chunk) for chunk in CHUNKS]
    blocks = {n: block(*n) for n in order}
    mine, summed = [], []
    for chunk in CHUNKS:
        arrived = []
        for k in (2, 1, 3):
            arrived.append(lax.ppermute(blocks[k, chunk], "x", turn(X, k)))
        ready, kept = gather(blocks[0, chunk], *arrived, at)
        mine.append(kept)
        summed.append(exchanged(ready, "z"))
    before = []
    for n in CHUNKS[:-1]:
        before += first(mine[n], summed[n], at, weight)
    *tiles, squares = last(mine[-1], summed[-1], before, at, weight)
    arrived = [lax.ppermute(tiles[k], "dp", turn(DP, k)) for k in range(1, DP)]
    kept = keep(tiles[0])
    squares = exchanged(squares, ("z", "core"))
    squares = call(pass_kernel, jax.ShapeDtypeStruct((DP * X, 1, LANE), F32), [whole()], whole())(squares)
    shape = jax.ShapeDtypeStruct((DP, LANE, outs // DP), F32)
    blocks = call(upright_kernel, shape, [whole()] * DP, whole())(kept, *arrived)
    squares = exchanged(squares, ("dp", "x"))
    clip_bound = math.sqrt(features * outs)
    return call(
        functools.partial(combine_kernel, clip_bound),
        jax.ShapeDtypeStruct((LANE, outs // DP), F32),
        [whole()] * 2,
        whole(),
        scalars=1,
    )(at, squares, blocks)


def solution(mesh):
    fine = Mesh(mesh.devices.reshape(DP, X, Z, CORE), ("dp", "x", "z", "core"))
    ctx = ("x", "z", "core")
    in_specs = (P("dp", ctx, None), P(), P("dp", ctx, None), P("dp"))
    out_specs = P(ctx, "dp")
    return jax.shard_map(
        per_device, mesh=fine, in_specs=in_specs, out_specs=out_specs, check_vma=False
    )
```
